32 devices in a mesh: row: 4 (over z), col: 8 (over y, x, core).
Axes of the slice: x: 2, y: 2, z: 4, core: 2. Of those that a mesh axis runs over, the one named last changes fastest.
Arguments:
- inverse_interior: float32 [4, 8, 1536, 1536], P('row', 'col'), may hold values from -0.15625 to 0.15625
- coupling: float32 [4, 8, 1536, 1024], P('row', 'col'), may hold values from -1 to 1
- interface_block: float32 [4, 8, 1024, 1024], P('row', 'col'), may hold values from -6 to 6
- iface_ids: int32 [4, 8, 4], P('row', 'col'), may hold values from 0 to 7, as said below
- row_place: int32 [8], replicated, may hold values from 0 to 7, as said below
- col_place: int32 [8], replicated, may hold values from 0 to 7, as said below
Outputs:
- assembled: float32 [8, 256, 8, 256], P('row', None, 'col')
The draws below stay inside these ranges and needn't reach their ends.
Inputs may be any that keep to these rules, and one draw needn't show every extreme that they name: `row_place`: A permutation of the tile ids. `col_place`: a permutation of the tile ids; two ids whose values of row_place differ mod 4 have values of col_place that differ mod 8. `iface_ids`: the 4 ids of one subdomain have pairwise different row_place mod 4, hence pairwise different col_place mod 8.
All inputs are finite; a program needn't handle non-finite values.
Results may differ from the reference program's by a relative error of at most 0.0001.
Values sent between devices are 32-bit elements; how exact they have to be, the bound alone decides.
A program may use at most 192 MiB of HBM per device.

```python
import jax
import jax.numpy as jnp
from jax import lax

NG = 1024
TILE = 256
NI = 1536
OWN_R = 2
NB = 4
PROWS = 4
PCOLS = 8
NT = 8
OWN_C = 1


def layout(key):
    row_place = jax.random.permutation(jax.random.fold_in(key, 11), NT).astype(jnp.int32)
    position = jnp.arange(NT, dtype=jnp.int32)
    owner = row_place % PROWS
    scores = jax.random.permutation(jax.random.fold_in(key, 12), NT).astype(jnp.int32)
    same_owner = owner[:, None] == owner[None, :]
    ranking = jnp.sum(same_owner & (scores[None, :] < scores[:, None]), axis=1).astype(jnp.int32)
    spread = PCOLS // PROWS
    col_owner = owner * spread + ranking % spread
    col_place = (ranking // spread * PCOLS + col_owner).astype(jnp.int32)
    inverse = jnp.zeros((NT,), jnp.int32).at[row_place].set(position)
    devices = PROWS * PCOLS
    weights = jax.random.randint(jax.random.fold_in(key, 13), (devices, PROWS), 0, 1 << 20).astype(jnp.int32)
    weights = weights * PROWS + jnp.arange(PROWS, dtype=jnp.int32)[None, :]
    owners = jnp.argsort(weights, axis=1)[:, :NB].astype(jnp.int32)
    slot_draw = jax.random.randint(jax.random.fold_in(key, 14), (devices, NB), 0, OWN_R).astype(jnp.int32)
    global_ids = inverse[slot_draw * PROWS + owners].astype(jnp.int32)
    return (row_place, col_place, global_ids.reshape(PROWS, PCOLS, NB))


def draw_row_place(key, part):
    return layout(key)[0]


def draw_col_place(key, part):
    return layout(key)[1]


def draw_iface_ids(key, part):
    return layout(key)[2]


def level_of(stream_key, shape, shards, smallest, top_value):
    factor_of, own = 1.0, jax.random.fold_in(stream_key, 6)
    for dim, parts in shards:
        heights = jnp.exp(jax.random.uniform(jax.random.fold_in(own, dim), (parts,), jnp.float32, smallest / len(shards), top_value / len(shards)))
        factor_of = factor_of * jnp.repeat(heights, shape[dim] // parts).reshape([-1 if axis == dim else 1 for axis in range(len(shape))])
    return factor_of


def noise(key, extent, width, reach, split=(), kind=jnp.bfloat16):
    factor_of = level_of(key, extent, split, -0.22, 0.18) if split else 1.0
    values = jax.random.normal(key, extent, jnp.float32) * width * factor_of
    return jnp.minimum(jnp.maximum(values, -reach), reach).astype(kind)


def setup_inputs(seed: int = 0) -> dict:
    key_list = jax.random.split(jax.random.key(seed), 7)
    return {
        "inverse_interior": noise(key_list[0], (PROWS, PCOLS, NI, NI), NI ** -0.5, 0.15625, ((0, 4), (1, 8)), jnp.float32),
        "coupling": noise(key_list[1], (PROWS, PCOLS, NI, NG), 0.16, 1.0, ((0, 4), (1, 8)), jnp.float32),
        "interface_block": noise(key_list[2], (PROWS, PCOLS, NG, NG), 1.0, 6.0, ((0, 4), (1, 8)), jnp.float32),
        "iface_ids": draw_iface_ids(jax.random.fold_in(key_list[6], 71), 0),
        "row_place": draw_row_place(jax.random.fold_in(key_list[6], 71), 0),
        "col_place": draw_col_place(jax.random.fold_in(key_list[6], 71), 0),
    }


def reference(inverse_interior, coupling, interface_block, iface_ids, row_place, col_place):
    highest = lax.Precision.HIGHEST
    out_rows = ((row_place % PROWS) * OWN_R + row_place // PROWS).astype(jnp.int32)
    out_cols = ((col_place % PCOLS) * OWN_C + col_place // PCOLS).astype(jnp.int32)
    tile_count = NG // TILE
    devices = PROWS * PCOLS

    def absorb(accum, items):
        inverse, couple, block, global_ids = items
        solved = jnp.dot(inverse, couple, precision=highest, preferred_element_type=jnp.float32)
        product = lax.dot_general(couple, solved, (((0,), (0,)), ((), ())), precision=highest, preferred_element_type=jnp.float32)
        schur_block = block - product
        tile_grid = schur_block.reshape(tile_count, TILE, tile_count, TILE).transpose(0, 2, 1, 3)
        row_index = out_rows[global_ids]
        col_index = out_cols[global_ids]
        accum = accum.at[row_index[:, None], :, col_index[None, :], :].add(tile_grid)
        return accum, None

    items = (inverse_interior.reshape(devices, NI, NI), coupling.reshape(devices, NI, NG), interface_block.reshape(devices, NG, NG), iface_ids.reshape(devices, NB))
    initial = jnp.zeros((NT, TILE, NT, TILE), jnp.float32)
    accum, ignored = lax.scan(absorb, initial, items)
    return accum
```

```python
import jax
import jax.numpy as jnp
from jax import lax
from jax.sharding import PartitionSpec as P

TILE = 256


def on_device(inverse_interior, coupling, interface_block, iface_ids, row_place, col_place):
    high = lax.Precision.HIGH
    f32 = jnp.float32
    rows = lax.axis_size("row")
    cols = lax.axis_size("col")
    total_ids = row_place.shape[0]
    slots = total_ids // rows
    own_cols = total_ids // cols
    spread = cols // rows
    part = TILE // spread
    count = coupling.shape[3] // TILE
    c = coupling[0, 0]
    solved = jnp.dot(inverse_interior[0, 0], c, precision=high, preferred_element_type=f32)
    product = lax.dot_general(c, solved, (((0,), (0,)), ((), ())), precision=high, preferred_element_type=f32)
    schur = interface_block[0, 0] - product
    ids = iface_ids[0, 0]
    matches = ids[:, None] == jnp.arange(total_ids, dtype=jnp.int32)[None, :]
    pos = jnp.sum(jnp.where(matches, row_place[None, :], 0), axis=1)
    group = pos % rows
    hit = group[None, :] == jnp.arange(rows, dtype=jnp.int32)[:, None]
    local = jnp.sum(jnp.where(hit, jnp.arange(count, dtype=jnp.int32)[None, :], 0), axis=1)
    slot = jnp.sum(jnp.where(hit, pos[None, :] // rows + 1, 0), axis=1) - 1
    strips = jnp.stack([lax.dynamic_slice_in_dim(schur, local[p] * TILE, TILE, 0) for p in range(rows)])
    out = jnp.stack([lax.dynamic_slice_in_dim(strips, local[q] * TILE, TILE, 2) for q in range(rows)])
    out = out.reshape(rows, rows, spread, part, TILE).transpose(0, 2, 1, 3, 4).reshape(cols, rows, part, TILE)
    arrived = lax.all_to_all(out, "col", split_axis=0, concat_axis=0, tiled=True)
    codes = lax.all_gather(slot.astype(f32), "col")
    mine = lax.axis_index("col") // spread
    own_code = jnp.sum(jnp.where(jnp.arange(rows)[None, :] == mine, codes, 0.0), axis=1)
    table = jnp.arange(slots).astype(f32)
    row_hit = codes[:, :, None] == table
    col_hit = own_code[:, None] == table
    mask = row_hit[:, :, :, None] & col_hit[:, None, None, :]
    total = jnp.sum(
        jnp.where(mask[:, :, :, :, None, None], arrived[:, :, None, None], 0.0), axis=0
    )
    summed = lax.psum_scatter(total, "row", scatter_dimension=0, tiled=True)[0]
    gathered = lax.all_gather(summed, "col")
    gathered = gathered.reshape(rows, spread, slots, slots, part, TILE)
    pieces = []
    for u in range(own_cols):
        want = u * cols + lax.axis_index("col")
        place = jnp.sum(jnp.where(col_place == want, row_place, 0))
        piece = lax.dynamic_slice(
            gathered,
            (place % rows, 0, 0, place // rows, 0, 0),
            (1, spread, slots, 1, part, TILE),
        )
        pieces.append(piece[0, :, :, 0].transpose(1, 0, 2, 3).reshape(slots, TILE, TILE))
    return jnp.stack(pieces, axis=2)


def solution(mesh):
    return jax.shard_map(
        on_device,
        mesh=mesh,
        in_specs=(
            P("row", "col", None, None),
            P("row", "col", None, None),
            P("row", "col", None, None),
            P("row", "col", None),
            P(),
            P(),
        ),
        out_specs=P("row", None, "col", None),
        check_vma=False,
    )
```

```python
import functools

import jax
import jax.numpy as jnp
from jax import lax
from jax.experimental import pallas as pl
from jax.experimental.pallas import tpu as pltpu
from jax.sharding import PartitionSpec as P

TILE = 256


def general(inverse_interior, coupling, interface_block, iface_ids, row_place, col_place):
    high = lax.Precision.HIGH
    f32 = jnp.float32
    rows = lax.axis_size("row")
    cols = lax.axis_size("col")
    total_ids = row_place.shape[0]
    slots = total_ids // rows
    own_cols = total_ids // cols
    spread = cols // rows
    part = TILE // spread
    count = coupling.shape[3] // TILE
    c = coupling[0, 0]
    solved = jnp.dot(inverse_interior[0, 0], c, precision=high, preferred_element_type=f32)
    product = lax.dot_general(c, solved, (((0,), (0,)), ((), ())), precision=high, preferred_element_type=f32)
    schur = interface_block[0, 0] - product
    ids = iface_ids[0, 0]
    matches = ids[:, None] == jnp.arange(total_ids, dtype=jnp.int32)[None, :]
    pos = jnp.sum(jnp.where(matches, row_place[None, :], 0), axis=1)
    group = pos % rows
    hit = group[None, :] == jnp.arange(rows, dtype=jnp.int32)[:, None]
    local = jnp.sum(jnp.where(hit, jnp.arange(count, dtype=jnp.int32)[None, :], 0), axis=1)
    slot = jnp.sum(jnp.where(hit, pos[None, :] // rows + 1, 0), axis=1) - 1
    strips = jnp.stack([lax.dynamic_slice_in_dim(schur, local[p] * TILE, TILE, 0) for p in range(rows)])
    out = jnp.stack([lax.dynamic_slice_in_dim(strips, local[q] * TILE, TILE, 2) for q in range(rows)])
    out = out.reshape(rows, rows, spread, part, TILE).transpose(0, 2, 1, 3, 4).reshape(cols, rows, part, TILE)
    arrived = lax.all_to_all(out, "col", split_axis=0, concat_axis=0, tiled=True)
    codes = lax.all_gather(slot.astype(f32), "col")
    mine = lax.axis_index("col") // spread
    own_code = jnp.sum(jnp.where(jnp.arange(rows)[None, :] == mine, codes, 0.0), axis=1)
    table = jnp.arange(slots).astype(f32)
    row_hit = codes[:, :, None] == table
    col_hit = own_code[:, None] == table
    mask = row_hit[:, :, :, None] & col_hit[:, None, None, :]
    total = jnp.sum(
        jnp.where(mask[:, :, :, :, None, None], arrived[:, :, None, None], 0.0), axis=0
    )
    summed = lax.psum_scatter(total, "row", scatter_dimension=0, tiled=True)[0]
    gathered = lax.all_gather(summed, "col")
    gathered = gathered.reshape(rows, spread, slots, slots, part, TILE)
    pieces = []
    for u in range(own_cols):
        want = u * cols + lax.axis_index("col")
        place = jnp.sum(jnp.where(col_place == want, row_place, 0))
        piece = lax.dynamic_slice(
            gathered,
            (place % rows, 0, 0, place // rows, 0, 0),
            (1, spread, slots, 1, part, TILE),
        )
        pieces.append(piece[0, :, :, 0].transpose(1, 0, 2, 3).reshape(slots, TILE, TILE))
    return jnp.stack(pieces, axis=2)


def assemble(
    rows, cols, slots, own_cols,
    place_ref, code_ref, th_ref, tl_ref, ch_ref, cl_ref, block_ref,
    out_ref,
    tiles, landed, codes, acc, row_landed, final, stage, pair_landed,
    code_send, code_recv, tile_send, tile_recv, row_send, row_recv, all_send, all_recv, pair_send, pair_recv,
):
    spread = cols // rows
    part = TILE // spread
    groups = part // 8
    z = lax.axis_index("row")
    d = lax.axis_index("col")
    mine = lax.div(d, spread)
    k = lax.rem(d, spread)

    def remote(src, dst, send, recv, row, col):
        return pltpu.make_async_remote_copy(
            src_ref=src, dst_ref=dst, send_sem=send, recv_sem=recv,
            device_id=(row, col), device_id_type=pl.DeviceIdType.MESH,
        )

    barrier = pltpu.get_barrier_semaphore()
    for o in range(1, cols):
        pl.semaphore_signal(
            barrier, inc=1, device_id=(z, lax.rem(d + o, cols)), device_id_type=pl.DeviceIdType.MESH
        )
    for o in range(1, rows):
        pl.semaphore_signal(
            barrier, inc=1, device_id=(lax.rem(z + o, rows), d), device_id_type=pl.DeviceIdType.MESH
        )

    started = []
    code_copies = {}
    tile_copies = {}
    for j in range(rows):
        p = lax.rem(z + 1 + j, rows)
        strip = pl.ds(pl.multiple_of(p * TILE, TILE), TILE)

        @pl.loop(0, rows)
        def _(q, j=j, strip=strip):
            band = pl.ds(pl.multiple_of(q * TILE, TILE), TILE)
            f32 = jnp.float32
            product = (
                jnp.dot(tl_ref[strip, :], ch_ref[:, band], preferred_element_type=f32)
                + jnp.dot(th_ref[strip, :], cl_ref[:, band], preferred_element_type=f32)
                + jnp.dot(th_ref[strip, :], ch_ref[:, band], preferred_element_type=f32)
            )
            tile = block_ref[strip, band] - product
            tiles[j, pl.ds(q * spread, spread)] = tile.reshape(spread, groups, 8, TILE)

        if j == 0:
            pl.semaphore_wait(barrier, cols + rows - 2)
            for o in range(1, cols):
                copy = remote(
                    code_ref, codes.at[o], code_send.at[o], code_recv.at[o], z, lax.rem(d + o, cols)
                )
                copy.start()
                code_copies[o] = copy
                started.append(copy)
        for o in range(1, cols):
            other = lax.rem(d + o, cols)
            copy = remote(
                tiles.at[j, other], landed.at[j, o], tile_send.at[j, o], tile_recv.at[j, o], z, other
            )
            copy.start()
            tile_copies[j, o] = copy
            started.append(copy)

    for o in range(1, cols):
        code_copies[o].wait_recv()
    row_copies = []
    step = min(4, groups)
    for j in range(rows):
        p = lax.rem(z + 1 + j, rows)
        for o in range(1, cols):
            tile_copies[j, o].wait_recv()

        @pl.loop(0, groups // step)
        def _(i, j=j, p=p):
            span = pl.ds(i * step, step)
            sums = {}
            for o in range(cols):
                x = tiles[j, d, span] if o == 0 else landed[j, o, span]
                code = code_ref if o == 0 else codes.at[o]
                row_code, col_code = code[p], code[mine]
                for t in range(slots):
                    for s in range(slots):
                        here = (row_code == float(s)) & (col_code == float(t))
                        term = jnp.where(here[None], x, 0.0)
                        sums[t, s] = sums[t, s] + term if o else term
            for t in range(slots):
                for s in range(slots):
                    acc[j, t, s, span] = sums[t, s]

        if j < rows - 1:
            copy = remote(acc.at[j], row_landed.at[j], row_send.at[j], row_recv.at[j], p, d)
            copy.start()
            row_copies.append(copy)
            started.append(copy)

    for copy in row_copies:
        copy.wait_recv()
    for t in range(slots):
        for s in range(slots):

            @pl.loop(0, groups // step)
            def _(i, t=t, s=s):
                span = pl.ds(i * step, step)
                value = acc[rows - 1, t, s, span]
                for j in range(rows - 1):
                    value = value + row_landed[j, t, s, span]
                final[0, t, s, span] = value

    all_copies = []
    for o in range(1, rows):
        other = lax.rem(mine + o, rows) * spread + k
        copy = remote(final.at[0], final.at[o], all_send.at[o], all_recv.at[o], z, other)
        copy.start()
        all_copies.append(copy)
        started.append(copy)
    for copy in all_copies:
        copy.wait_recv()

    def column(u, c):
        place = place_ref[u * cols + c]
        value = None
        for o in range(rows):
            owner = lax.rem(mine - o + rows, rows)
            for t in range(slots):
                here = place == (owner + t * rows).astype(jnp.float32)
                term = jnp.where(here[None, None], final[o, t], 0.0)
                value = term if value is None else value + term
        return value

    pair_copies = {}
    for n in range(1, spread):
        other = mine * spread + lax.rem(k + n, spread)
        for u in range(own_cols):
            stage[n, u] = column(u, other)
        copy = remote(stage.at[n], pair_landed.at[n], pair_send.at[n], pair_recv.at[n], z, other)
        copy.start()
        pair_copies[n] = copy
        started.append(copy)
    for u in range(own_cols):
        out_ref[u, :, k] = column(u, d)
    for n in range(1, spread):
        pair_copies[n].wait_recv()
        source = lax.rem(k - n + spread, spread)
        for u in range(own_cols):
            out_ref[u, :, source] = pair_landed[n, u]
    for copy in started:
        copy.wait_send()


def split(x):
    high = lax.reduce_precision(x, 8, 7)
    return high.astype(jnp.bfloat16), (x - high).astype(jnp.bfloat16)


def on_device(inverse_interior, coupling, interface_block, iface_ids, row_place, col_place):
    f32 = jnp.float32
    rows = lax.axis_size("row")
    cols = lax.axis_size("col")
    count = coupling.shape[3] // TILE
    if rows != count:
        return general(inverse_interior, coupling, interface_block, iface_ids, row_place, col_place)
    total_ids = row_place.shape[0]
    slots = total_ids // rows
    own_cols = total_ids // cols
    spread = cols // rows
    part = TILE // spread
    groups = part // 8
    ids = iface_ids[0, 0]
    matches = ids[:, None] == jnp.arange(total_ids, dtype=jnp.int32)[None, :]
    pos = jnp.sum(jnp.where(matches, row_place[None, :], 0), axis=1)
    hit = (pos % rows)[None, :] == jnp.arange(rows, dtype=jnp.int32)[:, None]
    local = jnp.sum(jnp.where(hit, jnp.arange(count, dtype=jnp.int32)[None, :], 0), axis=1)
    slot = jnp.sum(jnp.where(hit, pos[None, :] // rows, 0), axis=1)
    starts = [local[q] * TILE for q in range(rows)]

    def sort(x, axis):
        return jnp.concatenate([lax.dynamic_slice_in_dim(x, at, TILE, axis) for at in starts], axis)

    c = sort(coupling[0, 0], 1)
    block = sort(sort(interface_block[0, 0], 0), 1)
    left = lax.dot_general(
        c, inverse_interior[0, 0], (((0,), (0,)), ((), ())),
        precision=lax.Precision.HIGH, preferred_element_type=f32,
    )
    th, tl = split(left)
    ch, cl = split(c)
    code = jnp.broadcast_to(slot.astype(f32)[:, None, None], (rows, 8, TILE))
    order = jnp.arange(total_ids, dtype=jnp.int32)
    place = jnp.sum(jnp.where(order[:, None] == col_place[None, :], row_place[None, :], 0), axis=1)
    place = jnp.broadcast_to(place.astype(f32)[:, None, None], (total_ids, 8, TILE))
    vmem = pl.BlockSpec(memory_space=pltpu.VMEM)
    dma = pltpu.SemaphoreType.DMA
    out = pl.pallas_call(
        functools.partial(assemble, rows, cols, slots, own_cols),
        out_shape=jax.ShapeDtypeStruct((own_cols, slots, spread, groups, 8, TILE), f32),
        in_specs=[vmem] * 7,
        out_specs=vmem,
        scratch_shapes=[
            pltpu.VMEM((rows, cols, groups, 8, TILE), f32),
            pltpu.VMEM((rows, cols, groups, 8, TILE), f32),
            pltpu.VMEM((cols, rows, 8, TILE), f32),
            pltpu.VMEM((rows, slots, slots, groups, 8, TILE), f32),
            pltpu.VMEM((rows, slots, slots, groups, 8, TILE), f32),
            pltpu.VMEM((rows, slots, slots, groups, 8, TILE), f32),
            pltpu.VMEM((spread, own_cols, slots, groups, 8, TILE), f32),
            pltpu.VMEM((spread, own_cols, slots, groups, 8, TILE), f32),
            dma((cols,)), dma((cols,)), dma((rows, cols)), dma((rows, cols)),
            dma((rows,)), dma((rows,)), dma((rows,)), dma((rows,)), dma((spread,)), dma((spread,)),
        ],
        compiler_params=pltpu.CompilerParams(collective_id=0, has_side_effects=True),
    )(place, code, th, tl, ch, cl, block)
    return out.reshape(own_cols, slots, TILE, TILE).transpose(1, 2, 0, 3)


def solution(mesh):
    return jax.shard_map(
        on_device,
        mesh=mesh,
        in_specs=(
            P("row", "col", None, None),
            P("row", "col", None, None),
            P("row", "col", None, None),
            P("row", "col", None),
            P(),
            P(),
        ),
        out_specs=P("row", None, "col", None),
        check_vma=False,
    )
```
